8 devices in a mesh: inst: 1 (over z), qy: 2 (over y), qx: 4 (over x, core).
Axes of the slice: x: 2, y: 2, z: 1, core: 2. Of those that a mesh axis runs over, the one named last changes fastest.
Arguments:
- cost_diag: float32 [32768], P(('inst', 'qx', 'qy'))
- gamma_angles: float32 [4], replicated
- beta_angles: float32 [4], replicated
Outputs:
- output 1: float32 [1], P('inst')
- output 2: float32 [32768], P(('inst', 'qx', 'qy'))
- output 3: float32 [32768], P(('inst', 'qx', 'qy'))
All inputs are finite; a program needn't handle non-finite values.
Results may differ from the reference program's by a relative error of at most 0.001.
Values sent between devices are 32-bit elements.
A program may use at most 1 GiB of HBM per device.

```python
import math
import jax
import jax.numpy as jnp
from jax import lax

NQUBITS = 15
LAYERS = 4
DEGREE = 2

STATE_LEN = 2 ** NQUBITS
NUM_EDGES = DEGREE * NQUBITS // 2
EXTRA_EDGES = NUM_EDGES - NQUBITS


def draw_edges(key):
    key_first, key_ends, key_step = jax.random.split(key, 3)
    first_ends = jnp.arange(NQUBITS, dtype=jnp.int32)
    first_other = (first_ends + 1 + jax.random.randint(key_first, (NQUBITS,), 0, NQUBITS - 1, dtype=jnp.int32)) % NQUBITS
    extra_ends = jax.random.randint(key_ends, (EXTRA_EDGES,), 0, NQUBITS, dtype=jnp.int32)
    extra_other = (extra_ends + 1 + jax.random.randint(key_step, (EXTRA_EDGES,), 0, NQUBITS - 1, dtype=jnp.int32)) % NQUBITS
    return jnp.concatenate([first_ends, extra_ends]), jnp.concatenate([first_other, extra_other])


def cut_values(ends_a, ends_b, weights):
    index_bits = jnp.arange(STATE_LEN, dtype=jnp.int32)

    def add_edge(edge_idx, cut_sum):
        bit_a = jnp.right_shift(index_bits, ends_a[edge_idx]) & 1
        bit_b = jnp.right_shift(index_bits, ends_b[edge_idx]) & 1
        return cut_sum + weights[edge_idx] * (bit_a ^ bit_b).astype(jnp.float32)

    cut_sum = lax.fori_loop(0, NUM_EDGES, add_edge, jnp.zeros((STATE_LEN,), jnp.float32))
    return cut_sum / math.sqrt(NUM_EDGES)


def setup_inputs(seed: int = 0, part: int = 0) -> dict:
    part_key = jax.random.fold_in(jax.random.key(seed), part)
    key_edges, key_weights = jax.random.split(part_key)
    ends_a, ends_b = draw_edges(key_edges)
    weights = jax.random.uniform(key_weights, (NUM_EDGES,), jnp.float32, 0.5, 1.5)
    key_gamma, key_beta = jax.random.split(jax.random.key(seed + 1))
    gamma_angles = jax.random.uniform(key_gamma, (LAYERS,), jnp.float32, 0.3, 1.0)
    beta_angles = jax.random.uniform(key_beta, (LAYERS,), jnp.float32, 0.4, 1.2)
    return {'cost_diag': cut_values(ends_a, ends_b, weights), 'gamma_angles': gamma_angles, 'beta_angles': beta_angles}


def mixer_gate(amp_re, amp_im, qubit_idx, cos_half, sin_half):
    block_shape = (-1, 2, 2 ** qubit_idx)
    re_blocks = amp_re.reshape(block_shape)
    im_blocks = amp_im.reshape(block_shape)
    new_re = cos_half * re_blocks + sin_half * jnp.flip(im_blocks, axis=1)
    new_im = cos_half * im_blocks - sin_half * jnp.flip(re_blocks, axis=1)
    return new_re.reshape(-1), new_im.reshape(-1)


def reference(cost_diag, gamma_angles, beta_angles):
    start_amp = 2.0 ** (-NQUBITS / 2.0)
    amp_re = jnp.full((STATE_LEN,), start_amp, jnp.float32)
    amp_im = jnp.zeros((STATE_LEN,), jnp.float32)

    def layer_step(layer_state, angles):
        amp_re, amp_im = layer_state
        gamma_one, beta_one = angles
        phase_arg = gamma_one * cost_diag
        cos_t = jnp.cos(phase_arg)
        sin_t = jnp.sin(phase_arg)
        amp_re, amp_im = amp_re * cos_t + amp_im * sin_t, amp_im * cos_t - amp_re * sin_t
        cos_half = jnp.cos(0.5 * beta_one)
        sin_half = jnp.sin(0.5 * beta_one)
        for qubit_idx in range(NQUBITS):
            amp_re, amp_im = mixer_gate(amp_re, amp_im, qubit_idx, cos_half, sin_half)
        return (amp_re, amp_im), None

    (amp_re, amp_im), _unused = lax.scan(layer_step, (amp_re, amp_im), (gamma_angles, beta_angles))
    energy = jnp.sum(cost_diag * (amp_re * amp_re + amp_im * amp_im)).reshape(1)
    return energy, amp_re, amp_im
```

```python
import functools
import math

import jax
import jax.numpy as jnp
from jax import lax
from jax.experimental import pallas as pl
from jax.experimental.pallas import tpu as pltpu
from jax.sharding import PartitionSpec as P

MESH = pl.DeviceIdType.MESH
ROWS, LANES = 32, 128
F32 = jnp.float32


def gather_kernel(cost_ref, all_ref, local_sem, send_sem, recv_sem):
    qx, qy = lax.axis_index('qx'), lax.axis_index('qy')
    other_y = 1 - qy
    other_c = qx + 1 - 2 * lax.rem(qx, 2)
    peers = [{'qx': qx, 'qy': other_y}, {'qx': other_c, 'qy': qy}, {'qx': other_c, 'qy': other_y}]
    barrier = pltpu.get_barrier_semaphore()
    for peer in peers:
        pl.semaphore_signal(barrier, inc=1, device_id=peer, device_id_type=MESH)
    local = pltpu.make_async_copy(cost_ref, all_ref.at[0], local_sem)
    local.start()
    pl.semaphore_wait(barrier, 3)
    local.wait()
    copies = []
    for k, peer in enumerate(peers):
        copies.append(pltpu.make_async_remote_copy(
            src_ref=all_ref.at[0], dst_ref=all_ref.at[k + 1],
            send_sem=send_sem.at[k], recv_sem=recv_sem.at[k],
            device_id=peer, device_id_type=MESH))
    for copy in copies:
        copy.start()
    for copy in copies:
        copy.wait()


INV_2PI = 0.15915494309189535
P1, P2, P3 = 6.28125, 1.9350051879882812e-3, 3.0199159819568e-7


def sincos(x):
    n = jnp.round(x * INV_2PI)
    t = (((x - n * P1) - n * P2) - n * P3) * 0.25
    z = t * t
    s = ((-1.9515295891e-4 * z + 8.3321608736e-3) * z - 1.6666654611e-1) * z * t + t
    c = ((2.443315711809948e-5 * z - 1.388731625493765e-3) * z + 4.166664568298827e-2) * (z * z) + (1.0 - 0.5 * z)
    for _ in range(2):
        d = s + s
        c, s = 1.0 - d * s, d * c
    return c, s


def flip(x, mask):
    idx = lax.broadcasted_iota(jnp.int32, x.shape, 0) ^ mask
    return jnp.take_along_axis(x, idx, axis=0)


def pair_mix(re, im, i, j, cb, sb):
    re, im = list(re), list(im)
    for v in range(len(re)):
        if v & (1 << i) or v & (1 << j):
            continue
        a, b, c, d = v, v | 1 << i, v | 1 << j, v | 1 << i | 1 << j
        pr, pi = re[a] + re[d], im[a] + im[d]
        mr, mi = re[a] - re[d], im[a] - im[d]
        qr, qi = re[b] + re[c], im[b] + im[c]
        nr, ni = re[b] - re[c], im[b] - im[c]
        ur, ui = cb * pr + sb * qi, cb * pi - sb * qr
        vr, vi = cb * qr + sb * pi, cb * qi - sb * pr
        re[a], im[a], re[d], im[d] = ur + mr, ui + mi, ur - mr, ui - mi
        re[b], im[b], re[c], im[c] = vr + nr, vi + ni, vr - nr, vi - ni
    return re, im


def sublane_mix(re, im, c, s, cb, sb):
    out_re, out_im = [], []
    for r, i in zip(re, im):
        fr, fi = flip(r, 3), flip(i, 3)
        pr, pi, mr, mi = r + fr, i + fi, r - fr, i - fi
        qr, qi = flip(pr, 1), flip(pi, 1)
        r, i = (cb * pr + mr) + sb * qi, (cb * pi + mi) - sb * qr
        fr, fi = flip(r, 4), flip(i, 4)
        out_re.append(c * r + s * fi)
        out_im.append(c * i - s * fr)
    return out_re, out_im


def row_mix(re, im, c, s, cb, sb):
    re, im = pair_mix(re, im, 0, 1, cb, sb)
    re, im = pair_mix(re, im, 2, 3, cb, sb)
    return sublane_mix(re, im, 0.125 * c, 0.125 * s, cb, sb)


def transpose(blocks):
    whole = jnp.transpose(jnp.concatenate(blocks, axis=0))
    return [whole[8 * v:8 * v + 8] for v in range(16)]


def reverse_rows(blocks):
    return [flip(blocks[15 - v], 7) for v in range(16)]


def circuit_kernel(layers, amp0, cost_ref, gamma_ref, beta_ref, energy_ref, re_ref, im_ref):
    cost = [cost_ref[v // 4, 8 * (v % 4):8 * (v % 4) + 8, :] for v in range(16)]
    cost_t = transpose(cost)
    re = im = None
    for layer in range(layers):
        now = cost if layer % 2 == 0 else cost_t
        gamma = gamma_ref[layer]
        phases = [sincos(gamma * x) for x in now]
        if layer == 0:
            re, im = [amp0 * c for c, _ in phases], [-amp0 * s for _, s in phases]
        else:
            re, im = ([r * c + i * s for r, i, (c, s) in zip(re, im, phases)],
                      [i * c - r * s for r, i, (c, s) in zip(re, im, phases)])
        beta = jnp.full((8, LANES), beta_ref[layer], F32)
        c, s, cb, sb = jnp.cos(0.5 * beta), jnp.sin(0.5 * beta), jnp.cos(beta), jnp.sin(beta)
        re, im = row_mix(re, im, c, s, cb, sb)
        back_re, back_im = reverse_rows(re), reverse_rows(im)
        re, im = transpose(re), transpose(im)
        back_re, back_im = reverse_rows(transpose(back_re)), reverse_rows(transpose(back_im))
        re, im = ([c * r + s * b for r, b in zip(re, back_im)],
                  [c * i - s * b for i, b in zip(im, back_re)])
        re, im = row_mix(re, im, c, s, cb, sb)
    now = cost if layers % 2 == 0 else cost_t
    if layers % 2:
        re_n, im_n = transpose(re), transpose(im)
    else:
        re_n, im_n = re, im
    for v in range(4):
        re_ref[8 * v:8 * v + 8, :] = re_n[v]
        im_ref[8 * v:8 * v + 8, :] = im_n[v]
    terms = [x * (r * r + i * i) for x, r, i in zip(now, re, im)]
    while len(terms) > 1:
        terms = [a + b for a, b in zip(terms[::2], terms[1::2])]
    energy_ref[0] = 2.0 * jnp.sum(terms[0])


def solution(mesh):
    spec = P(('inst', 'qx', 'qy'))

    def device_body(cost, gamma, beta):
        layers = gamma.shape[0]
        vmem = pl.BlockSpec(memory_space=pltpu.VMEM)
        smem = pl.BlockSpec(memory_space=pltpu.SMEM)
        gathered = pl.pallas_call(
            gather_kernel,
            out_shape=jax.ShapeDtypeStruct((4, ROWS, LANES), F32),
            in_specs=[pl.BlockSpec(memory_space=pl.ANY)],
            out_specs=vmem,
            scratch_shapes=[pltpu.SemaphoreType.DMA, pltpu.SemaphoreType.DMA((3,)), pltpu.SemaphoreType.DMA((3,))],
            compiler_params=pltpu.CompilerParams(collective_id=0, has_side_effects=True),
            name='gather')(cost.reshape(ROWS, LANES))
        amp0 = 2.0 ** (-7.5)
        energy, re, im = pl.pallas_call(
            functools.partial(circuit_kernel, layers, amp0),
            out_shape=[jax.ShapeDtypeStruct((1,), F32)] + [jax.ShapeDtypeStruct((ROWS, LANES), F32)] * 2,
            in_specs=[vmem, smem, smem],
            out_specs=[smem, vmem, vmem],
            name='circuit')(gathered, gamma, beta)
        return energy, re.reshape(-1), im.reshape(-1)

    return jax.shard_map(device_body, mesh=mesh, in_specs=(spec, P(), P()), out_specs=(P('inst'), spec, spec), check_vma=False)
```

```python
import functools
import math

import jax
import jax.numpy as jnp
from jax import lax
from jax.experimental import pallas as pl
from jax.experimental.pallas import tpu as pltpu
from jax.sharding import PartitionSpec as P

MESH = pl.DeviceIdType.MESH
ROWS, LANES = 32, 128
F32 = jnp.float32


def gather_kernel(cost_ref, all_ref, local_sem, send_sem, recv_sem):
    qx, qy = lax.axis_index('qx'), lax.axis_index('qy')
    other_y = 1 - qy
    other_c = qx + 1 - 2 * lax.rem(qx, 2)
    peers = [{'qx': qx, 'qy': other_y}, {'qx': other_c, 'qy': qy}, {'qx': other_c, 'qy': other_y}]
    barrier = pltpu.get_barrier_semaphore()
    for peer in peers:
        pl.semaphore_signal(barrier, inc=1, device_id=peer, device_id_type=MESH)
    local = pltpu.make_async_copy(cost_ref, all_ref.at[0], local_sem)
    local.start()
    pl.semaphore_wait(barrier, 3)
    local.wait()
    copies = []
    for k, peer in enumerate(peers):
        copies.append(pltpu.make_async_remote_copy(
            src_ref=all_ref.at[0], dst_ref=all_ref.at[k + 1],
            send_sem=send_sem.at[k], recv_sem=recv_sem.at[k],
            device_id=peer, device_id_type=MESH))
    for copy in copies:
        copy.start()
    for copy in copies:
        copy.wait()


INV_2PI = 0.15915494309189535
P1, P2, P3 = 6.28125, 1.9350051879882812e-3, 3.0199159819568e-7


def sincos(x):
    n = jnp.round(x * INV_2PI)
    t = (((x - n * P1) - n * P2) - n * P3) * 0.25
    z = t * t
    s = ((-1.9515295891e-4 * z + 8.3321608736e-3) * z - 1.6666654611e-1) * z * t + t
    c = ((2.443315711809948e-5 * z - 1.388731625493765e-3) * z + 4.166664568298827e-2) * (z * z) + (1.0 - 0.5 * z)
    for _ in range(2):
        d = s + s
        c, s = 1.0 - d * s, d * c
    return c, s


def flip(x, mask):
    idx = lax.broadcasted_iota(jnp.int32, x.shape, 0) ^ mask
    return jnp.take_along_axis(x, idx, axis=0)


def pair_mix(re, im, i, j, cb, sb):
    re, im = list(re), list(im)
    for v in range(len(re)):
        if v & (1 << i) or v & (1 << j):
            continue
        a, b, c, d = v, v | 1 << i, v | 1 << j, v | 1 << i | 1 << j
        pr, pi = re[a] + re[d], im[a] + im[d]
        mr, mi = re[a] - re[d], im[a] - im[d]
        qr, qi = re[b] + re[c], im[b] + im[c]
        nr, ni = re[b] - re[c], im[b] - im[c]
        ur, ui = cb * pr + sb * qi, cb * pi - sb * qr
        vr, vi = cb * qr + sb * pi, cb * qi - sb * pr
        re[a], im[a], re[d], im[d] = ur + mr, ui + mi, ur - mr, ui - mi
        re[b], im[b], re[c], im[c] = vr + nr, vi + ni, vr - nr, vi - ni
    return re, im


def sublane_mix(re, im, c, s, cb, sb):
    out_re, out_im = [], []
    for r, i in zip(re, im):
        fr, fi = flip(r, 3), flip(i, 3)
        pr, pi, mr, mi = r + fr, i + fi, r - fr, i - fi
        qr, qi = flip(pr, 1), flip(pi, 1)
        r, i = (cb * pr + mr) + sb * qi, (cb * pi + mi) - sb * qr
        fr, fi = flip(r, 4), flip(i, 4)
        out_re.append(c * r + s * fi)
        out_im.append(c * i - s * fr)
    return out_re, out_im


def row_mix(re, im, c, s, cb, sb):
    re, im = pair_mix(re, im, 0, 1, cb, sb)
    re, im = pair_mix(re, im, 2, 3, cb, sb)
    return sublane_mix(re, im, 0.125 * c, 0.125 * s, cb, sb)


def transpose(blocks):
    whole = jnp.transpose(jnp.concatenate(blocks, axis=0))
    return [whole[8 * v:8 * v + 8] for v in range(16)]


def reverse_rows(blocks):
    return [flip(blocks[15 - v], 7) for v in range(16)]


def circuit_kernel(layers, amp0, cost_ref, gamma_ref, beta_ref, energy_ref, re_ref, im_ref):
    cost = [cost_ref[v // 4, 8 * (v % 4):8 * (v % 4) + 8, :] for v in range(16)]
    cost_t = transpose(cost)
    re = im = None
    for layer in range(layers):
        now = cost if layer % 2 == 0 else cost_t
        gamma = gamma_ref[layer]
        phases = [sincos(gamma * x) for x in now]
        if layer == 0:
            re, im = [amp0 * c for c, _ in phases], [-amp0 * s for _, s in phases]
        else:
            re, im = ([r * c + i * s for r, i, (c, s) in zip(re, im, phases)],
                      [i * c - r * s for r, i, (c, s) in zip(re, im, phases)])
        beta = jnp.full((8, LANES), beta_ref[layer], F32)
        c, s, cb, sb = jnp.cos(0.5 * beta), jnp.sin(0.5 * beta), jnp.cos(beta), jnp.sin(beta)
        re, im = row_mix(re, im, c, s, cb, sb)
        back_re, back_im = reverse_rows(re), reverse_rows(im)
        re, im = transpose(re), transpose(im)
        back_re, back_im = reverse_rows(transpose(back_re)), reverse_rows(transpose(back_im))
        re, im = ([c * r + s * b for r, b in zip(re, back_im)],
                  [c * i - s * b for i, b in zip(im, back_re)])
        re, im = row_mix(re, im, c, s, cb, sb)
    now = cost if layers % 2 == 0 else cost_t
    if layers % 2:
        re_n, im_n = transpose(re), transpose(im)
    else:
        re_n, im_n = re, im
    for v in range(4):
        re_ref[8 * v:8 * v + 8, :] = re_n[v]
        im_ref[8 * v:8 * v + 8, :] = im_n[v]
    terms = [x * (r * r + i * i) for x, r, i in zip(now, re, im)]
    while len(terms) > 1:
        terms = [a + b for a, b in zip(terms[::2], terms[1::2])]
    energy_ref[0] = 2.0 * jnp.sum(terms[0])


def solution(mesh):
    spec = P(('inst', 'qx', 'qy'))

    def device_body(cost, gamma, beta):
        layers = gamma.shape[0]
        vmem = pl.BlockSpec(memory_space=pltpu.VMEM)
        smem = pl.BlockSpec(memory_space=pltpu.SMEM)
        gathered = pl.pallas_call(
            gather_kernel,
            out_shape=jax.ShapeDtypeStruct((4, ROWS, LANES), F32),
            in_specs=[pl.BlockSpec(memory_space=pltpu.HBM)],
            out_specs=vmem,
            scratch_shapes=[pltpu.SemaphoreType.DMA, pltpu.SemaphoreType.DMA((3,)), pltpu.SemaphoreType.DMA((3,))],
            compiler_params=pltpu.CompilerParams(collective_id=0, has_side_effects=True, vmem_limit_bytes=2 << 20),
            name='gather')(cost.reshape(ROWS, LANES))
        amp0 = 2.0 ** (-7.5)
        energy, re, im = pl.pallas_call(
            functools.partial(circuit_kernel, layers, amp0),
            out_shape=[jax.ShapeDtypeStruct((1,), F32)] + [jax.ShapeDtypeStruct((ROWS, LANES), F32)] * 2,
            in_specs=[vmem, smem, smem],
            out_specs=[smem, vmem, vmem],
            compiler_params=pltpu.CompilerParams(vmem_limit_bytes=4 << 20),
            name='circuit')(gathered, gamma, beta)
        return energy, re.reshape(-1), im.reshape(-1)

    return jax.shard_map(device_body, mesh=mesh, in_specs=(spec, P(), P()), out_specs=(P('inst'), spec, spec), check_vma=False)
```
